32 devices in a mesh: vtx: 8 (over z, x), src: 4 (over y, core).
Axes of the slice: x: 2, y: 2, z: 4, core: 2. Of those that a mesh axis runs over, the one named last changes fastest.
Arguments:
- heat: float32 [64, 64, 8192], P(None, ('vtx', 'src')), may hold values from -12 to 12
- cotan: float32 [4, 64, 8192], P(None, 'vtx'), may hold values from 0.2 to 2
- source_index: int32 [64], replicated, may hold values from 0 to 524287
Outputs:
- normalised: float32 [64, 64, 8192], P('src', 'vtx')
- col_norm: float32 [64], P('src')
The draws below stay inside these ranges and needn't reach their ends.
Inputs may be any that keep to these rules, and one draw needn't show every extreme that they name: `source_index`: row-major vertex indices, sources may share a vertex.
All inputs are finite; a program needn't handle non-finite values.
Results may differ from the reference program's by a relative error of at most 0.0003.
Values sent between devices are 32-bit elements; how exact they have to be, the bound alone decides.
A program may use at most 64 MiB of HBM per device.

```python
import math
import jax
import jax.numpy as jnp
from jax import lax

SOURCES = 64
GX = 8192
GY = 64


def draw_heat(key, part):
    rows = jnp.arange(GY, dtype=jnp.float32) / max(GY - 1, 1)
    base_key = jax.random.fold_in(key, 11)
    factor_key = jax.random.fold_in(key, 23)
    row_factor = jax.random.uniform(factor_key, (SOURCES, GY), jnp.float32, 0.3, 1.0)
    base = jnp.clip(jax.random.normal(base_key, (SOURCES, GY, GX), jnp.float32), -4.0, 4.0)
    scale = 1.0 + 2.0 * rows
    return base * (scale[None, :] * row_factor)[:, :, None]


def plant(entries, stream_key, smallest, top_value):
    longest = entries.shape.index(max(entries.shape))
    spots = []
    for shift in (0, 1):
        where = [jax.random.randint(jax.random.fold_in(stream_key, axis), (), 0, length) for axis, length in enumerate(entries.shape)]
        where[longest] = (where[longest] + shift) % entries.shape[longest]
        spots.append(tuple(where))
    return entries.at[spots[0]].set(smallest).at[spots[1]].set(top_value)


def shard_levels(rng, shape, cuts, least, largest):
    loudness, own = 1.0, jax.random.fold_in(rng, 6)
    for axis_at, blocks in cuts:
        heights = jnp.exp(jax.random.uniform(jax.random.fold_in(own, axis_at), (blocks,), jnp.float32, least / len(cuts), largest / len(cuts)))
        loudness = loudness * jnp.repeat(heights, shape[axis_at] // blocks).reshape([-1 if axis == axis_at else 1 for axis in range(len(shape))])
    return loudness


def setup_inputs(seed: int = 0) -> dict:
    streams_of = jax.random.split(jax.random.key(seed), 4)
    return {
        "heat": draw_heat(jax.random.fold_in(streams_of[3], 71), 0),
        "cotan": jnp.clip(jnp.exp(math.log(2.0) - 2.3025851 * jax.random.uniform(streams_of[1], (4, GY, GX), jnp.float32) ** shard_levels(streams_of[1], (4, GY, GX), ((1, 8),), -0.2, 0.2)), 0.2, 2.0),
        "source_index": plant(jax.random.randint(streams_of[2], (SOURCES,), 0, GY * GX), jax.random.fold_in(streams_of[2], 1), 0, (GY * GX) - 1).astype(jnp.int32),
    }


def from_right(values):
    return jnp.concatenate([values[..., 1:], jnp.zeros_like(values[..., :1])], axis=-1)

def from_left(values):
    return jnp.concatenate([jnp.zeros_like(values[..., :1]), values[..., :-1]], axis=-1)

def masked_cotan(cotan, row_start, total_rows):
    shape = cotan.shape[1:]
    rows = row_start + lax.broadcasted_iota(jnp.int32, shape, 0)
    cols = lax.broadcasted_iota(jnp.int32, shape, 1)
    inside_col = cols < shape[1] - 1
    inside_row = rows < total_rows - 1
    mass = cotan[0]
    east = jnp.where(inside_col, cotan[1], 0.0)
    north = jnp.where(inside_row, cotan[2], 0.0)
    diag = jnp.where(inside_col & inside_row, cotan[3], 0.0)
    return (mass, east, north, diag)

def stencil_defect(padded, mass, east, north_ext, diag_ext, row_start, sources, amplitude):
    center = padded[:, 1:-1, :]
    above = padded[:, 2:, :]
    below = padded[:, :-2, :]
    north = north_ext[1:]
    south_weight = north_ext[:-1]
    diag = diag_ext[1:]
    southwest_weight = from_left(diag_ext[:-1])
    west_weight = from_left(east)
    result = mass * center + east * (center - from_right(center))
    result = result + west_weight * (center - from_left(center))
    result = result + north * (center - above) + south_weight * (center - below)
    result = result + diag * (center - from_right(above)) + southwest_weight * (center - from_left(below))
    count_rows, width = (center.shape[1], center.shape[2])
    row_ids = row_start + lax.broadcasted_iota(jnp.int32, (count_rows, width), 0)
    col_ids = lax.broadcasted_iota(jnp.int32, (count_rows, width), 1)
    flat = row_ids * width + col_ids
    delta = (flat[None, :, :] == sources.astype(jnp.int32)[:, None, None]).astype(jnp.float32)
    return result - amplitude * delta

def reference(heat, cotan, source_index):
    total_rows, width = (heat.shape[1], heat.shape[2])
    amplitude = math.sqrt(total_rows * width) / 8.0
    mass, east, north, diag = masked_cotan(cotan, 0, total_rows)
    north_ext = jnp.concatenate([jnp.zeros((1, width), jnp.float32), north], axis=0)
    diag_ext = jnp.concatenate([jnp.zeros((1, width), jnp.float32), diag], axis=0)

    def single(inputs):
        field, source = inputs
        padded = jnp.pad(field[None], ((0, 0), (1, 1), (0, 0)))
        result = stencil_defect(padded, mass, east, north_ext, diag_ext, 0, source[None], amplitude)[0]
        return (result, jnp.sum(result * result))
    defect, squares = lax.map(single, (heat, source_index))
    norms = jnp.sqrt(squares / (total_rows * width) + 1e-06)
    return (defect / norms[:, None, None], norms)
```

```python
import functools
import math

import jax
import jax.numpy as jnp
from jax import lax
from jax.experimental import pallas as pl
from jax.experimental.pallas import tpu as pltpu
from jax.sharding import PartitionSpec as P

MESH = pl.DeviceIdType.MESH
F32 = jnp.float32
LANES = 128
ROWS = 8
TILES = 16
GROUP = 2


def kernel(
    n, nv, ng, width, pitch, amplitude,
    idx_ref, heat_ref, cot_ref, out_ref, norm_ref,
    H, X, R, D, W, cot, low, sq, G,
    load_sem, cot_sem, y_send, y_recv, z_send, z_recv, p_send, p_recv,
    h_send, h_recv, w_send, w_recv, s_send, s_recv, o_sem,
):
    v = lax.axis_index("vtx")
    src = lax.axis_index("src")
    nt = width // LANES
    k0, k1 = 2, ng // GROUP
    s0 = ng // k0
    total_rows = nv * ROWS
    far = list(range(2, n))
    upper = (src * 2) // n

    def peer(j):
        return ((src // 2 + j // 2) % (n // 2)) * 2 + (src + j) % 2

    def load(j):
        at = pl.ds(peer(j) * ng, ng)
        return pltpu.make_async_copy(heat_ref.at[at], H.at[at], load_sem.at[j])

    order = far + [0, 1]
    for j in order:
        load(j).start()
    cot_load = pltpu.make_async_copy(cot_ref, cot, cot_sem)
    cot_load.start()

    barrier = pltpu.get_barrier_semaphore()
    for j in range(1, n):
        pl.semaphore_signal(barrier, inc=1, device_id={"src": peer(j)}, device_id_type=MESH)

    @pl.loop(1, nv)
    def _(o):
        pl.semaphore_signal(barrier, inc=1, device_id={"vtx": (v + o) % nv}, device_id_type=MESH)

    def extract(j):
        load(j).wait()
        base = peer(j) * ng

        @pl.loop(0, ng)
        def _(s):
            for r in range(2):
                row = H[base + s, pl.ds(r, nt, stride=2), :]
                X[r, pl.ds(pl.multiple_of((base + s) * nt, nt), nt), :] = row

    for j in far:
        extract(j)

    pl.semaphore_wait(barrier, (n - 1) + (nv - 1))

    def row_copy(r, j, first, count, send, recv):
        start = pl.multiple_of((peer(j) * ng + first) * nt, nt)
        land = pl.multiple_of((1 + 2 * src + r) * pitch + first * nt, 8)
        return pltpu.make_async_remote_copy(
            src_ref=X.at[r, pl.ds(start, count * nt)],
            dst_ref=R.at[pl.ds(land, count * nt)],
            send_sem=send, recv_sem=recv,
            device_id={"src": peer(j)}, device_id_type=MESH,
        )

    def pass0(k, j):
        return row_copy(upper, j, k * s0, s0, y_send.at[j, k], y_recv.at[j, k])

    def pass1(k, j):
        return row_copy(1 - upper, j, k * GROUP, GROUP, z_send.at[j, k], z_recv.at[j, k])

    for k in range(k0):
        for j in far:
            pass0(k, j).start()

    @pl.loop(0, k1)
    def _(k):
        for j in far:
            pass1(k, j).start()

    def weight_copy():
        return pltpu.make_async_remote_copy(
            src_ref=cot_ref.at[pl.ds(2, 2)], dst_ref=low, send_sem=w_send, recv_sem=w_recv,
            device_id={"vtx": (v + 1) % nv}, device_id_type=MESH,
        )

    @pl.when(v < nv - 1)
    def _():
        weight_copy().start()

    extract(1)

    def partner(r):
        return row_copy(r, 1, 0, ng, p_send.at[r], p_recv.at[r])

    for r in range(2):
        partner(r).start()

    load(0).wait()

    @pl.loop(0, ng)
    def _(s):
        for r in range(2):
            row = H[src * ng + s, pl.ds(r, nt, stride=2), :]
            R[pl.ds(pl.multiple_of((1 + 2 * src + r) * pitch + s * nt, 8), nt), :] = row

    @pl.when(v == 0)
    def _():
        R[pl.ds(0, ng * nt), :] = jnp.zeros((ng * nt, LANES), F32)

    @pl.when(v == nv - 1)
    def _():
        R[pl.ds(9 * pitch, ng * nt), :] = jnp.zeros((ng * nt, LANES), F32)

    def halo(up, k):
        first = k * s0 * nt
        out = (8 if up else 1) * pitch + first
        land = (0 if up else 9) * pitch + first
        to = (v + 1) % nv if up else (v + nv - 1) % nv
        return pltpu.make_async_remote_copy(
            src_ref=R.at[pl.ds(out, s0 * nt)], dst_ref=R.at[pl.ds(land, s0 * nt)],
            send_sem=h_send.at[up, k], recv_sem=h_recv.at[up, k],
            device_id={"vtx": to}, device_id_type=MESH,
        )

    def weights():
        cot_load.wait()

        @pl.when(v > 0)
        def _():
            weight_copy().wait_recv()

        shape = (ROWS, width)
        rows = lax.broadcasted_iota(jnp.int32, shape, 0)
        cols = lax.broadcasted_iota(jnp.int32, shape, 1)
        inside_col = cols < width - 1
        inside_row = rows + v * ROWS < total_rows - 1
        last = rows == ROWS - 1
        below = jnp.broadcast_to(v > 0, shape)
        W[0] = jnp.where(inside_col, cot[1], 0.0)
        W[1] = jnp.where(inside_row, cot[2], 0.0)
        W[4] = jnp.where(inside_col & inside_row, cot[3], 0.0)
        W[2] = pltpu.roll(jnp.where(last, jnp.where(below, low[0], 0.0), W[1]), 1, 0)
        W[3] = pltpu.roll(jnp.where(last, jnp.where(below & inside_col, low[1], 0.0), W[4]), 1, 0)
        W[5] = pltpu.roll(W[0], 1, 1)
        W[6] = cot[0] + W[0] + W[5] + W[1] + W[2] + W[4] + pltpu.roll(W[3], 1, 1)
        W[4] = pltpu.roll(W[4], 1, 1)

    for r in range(2):
        partner(r).wait_recv()
    weights()
    for k in range(k0):
        for j in far:
            pass0(k, j).wait_recv()

        @pl.when(v < nv - 1)
        def _():
            halo(1, k).start()

        @pl.when(v > 0)
        def _():
            halo(0, k).start()

    lane = lax.broadcasted_iota(jnp.int32, (ROWS, LANES), 1)
    flat = lax.broadcasted_iota(jnp.int32, (ROWS, LANES), 0) * width + lane
    first_lane, last_lane = lane == 0, lane == LANES - 1

    def out_copy(k):
        at = pl.ds(k * GROUP, GROUP)
        return pltpu.make_async_copy(D.at[at], out_ref.at[at], o_sem.at[k])

    def chunk(k):
        for j in far:
            pass1(k, j).wait_recv()
        spots = [
            idx_ref[src * ng + k * GROUP + i] - v * (ROWS * width) for i in range(GROUP)
        ]

        def block(b, sums):
            sums = list(sums)
            t0 = b * TILES

            def weight(m, t):
                return W[m, :, pl.ds(pl.multiple_of(t * LANES, LANES), LANES)]

            before = (t0 + nt - 1) % nt
            after = (t0 + TILES) % nt
            tiles = [t0 + i for i in range(TILES)]
            for i in range(GROUP):
                base = (k * GROUP + i) * nt

                def field(shift, t):
                    return R[pl.ds((1 + shift) * pitch + base + t, ROWS, stride=pitch), :]

                mids = [field(0, t) for t in tiles]
                ups = [field(1, t) for t in tiles]
                downs = [field(-1, t) for t in tiles]
                p = [weight(5, t) * m + weight(4, t) * u for t, m, u in zip(tiles, mids, ups)]
                q = [weight(0, t) * m + weight(3, t) * d for t, m, d in zip(tiles, mids, downs)]
                p.append(weight(5, after) * field(0, after) + weight(4, after) * field(1, after))
                q.insert(0, weight(0, before) * field(0, before) + weight(3, before) * field(-1, before))
                for c, t in enumerate(tiles):
                    right = pltpu.roll(jnp.where(first_lane, p[c + 1], p[c]), LANES - 1, 1)
                    left = pltpu.roll(jnp.where(last_lane, q[c], q[c + 1]), 1, 1)
                    d = weight(6, t) * mids[c] - weight(1, t) * ups[c] - weight(2, t) * downs[c]
                    d = d - right - left
                    d = d - jnp.where(flat == spots[i] - t * LANES, F32(amplitude), F32(0.0))
                    sums[i] = sums[i] + d * d
                    D[k * GROUP + i, :, pl.ds(pl.multiple_of(t * LANES, LANES), LANES)] = d
            return tuple(sums)

        zero = jnp.zeros((ROWS, LANES), F32)
        sums = lax.fori_loop(0, nt // TILES, block, (zero,) * GROUP)
        for i in range(GROUP):
            sq[pl.ds(k * GROUP + i, 1), :] = jnp.sum(sums[i], axis=0, keepdims=True)
        out_copy(k).start()

    per = s0 // GROUP
    for k in range(k0):
        @pl.when(v > 0)
        def _():
            halo(1, k).wait_recv()

        @pl.when(v < nv - 1)
        def _():
            halo(0, k).wait_recv()

        @pl.loop(k * per, (k + 1) * per)
        def _(c):
            chunk(c)

    def share(to, slot):
        return pltpu.make_async_remote_copy(
            src_ref=sq, dst_ref=G.at[slot], send_sem=s_send.at[to], recv_sem=s_recv.at[slot],
            device_id={"vtx": to}, device_id_type=MESH,
        )

    @pl.loop(1, nv)
    def _(o):
        share((v + o) % nv, v).start()

    G[v] = sq[...]
    for j in far:
        for k in range(k0):
            pass0(k, j).wait_send()

        @pl.loop(0, k1)
        def _(k):
            pass1(k, j).wait_send()
    for r in range(2):
        partner(r).wait_send()

    @pl.when(v < nv - 1)
    def _():
        weight_copy().wait_send()
        for k in range(k0):
            halo(1, k).wait_send()

    @pl.when(v > 0)
    def _():
        for k in range(k0):
            halo(0, k).wait_send()

    @pl.loop(0, k1)
    def _(k):
        out_copy(k).wait()

    @pl.loop(1, nv)
    def _(o):
        share((v + o) % nv, (v + o) % nv).wait_recv()

    total = lax.fori_loop(0, nv, lambda i, t: t + G[i], jnp.zeros((ng, LANES), F32))
    total = jnp.sum(total, axis=1, keepdims=True)
    norms = jnp.sqrt(total / (total_rows * width) + 1e-06)
    norm_ref[...] = jnp.broadcast_to(norms, (ng, LANES))

    @pl.loop(1, nv)
    def _(o):
        share((v + o) % nv, v).wait_send()


def on_device(n, nv, heat, cotan, source_index):
    sources, rpd, width = heat.shape
    assert rpd == 2 and cotan.shape[1] == ROWS and n % 2 == 0
    ng = sources // n
    nt = width // LANES
    pitch = -(-(ng * nt) // 64) * 64 + 8
    amplitude = math.sqrt(ROWS * nv * width) / 8.0
    tiled = heat.reshape(sources, rpd, nt, LANES).transpose(0, 2, 1, 3)
    tiled = tiled.reshape(sources, rpd * nt, LANES)
    dma = pltpu.SemaphoreType.DMA
    k0, k1 = 2, ng // GROUP
    defect, norms = pl.pallas_call(
        functools.partial(kernel, n, nv, ng, width, pitch, amplitude),
        out_shape=(
            jax.ShapeDtypeStruct((ng, ROWS, width), F32),
            jax.ShapeDtypeStruct((ng, LANES), F32),
        ),
        in_specs=[
            pl.BlockSpec(memory_space=pltpu.SMEM),
            pl.BlockSpec(memory_space=pl.ANY),
            pl.BlockSpec(memory_space=pl.ANY),
        ],
        out_specs=(
            pl.BlockSpec(memory_space=pl.ANY),
            pl.BlockSpec(memory_space=pltpu.VMEM),
        ),
        scratch_shapes=[
            pltpu.VMEM((sources, rpd * nt, LANES), F32),
            pltpu.VMEM((rpd, sources * nt, LANES), F32),
            pltpu.VMEM((10 * pitch, LANES), F32),
            pltpu.VMEM((ng, ROWS, width), F32),
            pltpu.VMEM((7, ROWS, width), F32),
            pltpu.VMEM((4, ROWS, width), F32),
            pltpu.VMEM((2, ROWS, width), F32),
            pltpu.VMEM((ng, LANES), F32),
            pltpu.VMEM((nv, ng, LANES), F32),
            dma((n,)), dma,
            dma((n, k0)), dma((n, k0)), dma((n, k1)), dma((n, k1)),
            dma((2,)), dma((2,)), dma((2, k0)), dma((2, k0)),
            dma, dma, dma((nv,)), dma((nv,)), dma((k1,)),
        ],
        compiler_params=pltpu.CompilerParams(collective_id=0, has_side_effects=True),
    )(source_index, tiled, cotan)
    norms = norms[:, 0]
    return (defect / norms[:, None, None], norms)


def solution(mesh):
    n, nv = mesh.shape["src"], mesh.shape["vtx"]
    return jax.shard_map(
        functools.partial(on_device, n, nv),
        mesh=mesh,
        in_specs=(P(None, ("vtx", "src"), None), P(None, "vtx", None), P()),
        out_specs=(P("src", "vtx", None), P("src")),
        check_vma=False,
    )
```

```python
import functools
import math

import jax
import jax.numpy as jnp
from jax import lax
from jax.experimental import pallas as pl
from jax.experimental.pallas import tpu as pltpu
from jax.sharding import PartitionSpec as P

MESH = pl.DeviceIdType.MESH
F32 = jnp.float32
LANES = 128
ROWS = 8
BLOCK = 32
GROUP = 2


def kernel(
    n, nv, ng, width, pitch, amplitude,
    idx_hbm, heat_ref, cot_ref, D, norm_ref,
    idx_ref, H, X, R, W, cot, low, sq, G,
    idx_sem, load_sem, cot_sem, y_send, y_recv, z_send, z_recv, p_send, p_recv,
    h_send, h_recv, w_send, w_recv, s_send, s_recv,
):
    v = lax.axis_index("vtx")
    src = lax.axis_index("src")
    nt = width // LANES
    k0, k1 = 2, ng // GROUP + 1
    s0 = ng // k0
    total_rows = nv * ROWS
    far = list(range(2, n))
    upper = (src * 2) // n

    def peer(j):
        return ((src // 2 + j // 2) % (n // 2)) * 2 + (src + j) % 2

    def load(j, k):
        at = pl.ds(peer(j) * ng + k * s0, s0)
        return pltpu.make_async_copy(heat_ref.at[at], H.at[at], load_sem.at[j, k])

    for j_set in (far, [1, 0]):
        for k in range(k0):
            for j in j_set:
                load(j, k).start()
    cot_load = pltpu.make_async_copy(cot_ref, cot, cot_sem)
    cot_load.start()
    idx_load = pltpu.make_async_copy(idx_hbm, idx_ref, idx_sem)
    idx_load.start()

    barrier = pltpu.get_barrier_semaphore()
    for j in range(1, n):
        pl.semaphore_signal(barrier, inc=1, device_id={"src": peer(j)}, device_id_type=MESH)

    @pl.loop(1, nv)
    def _(o):
        pl.semaphore_signal(barrier, inc=1, device_id={"vtx": (v + o) % nv}, device_id_type=MESH)

    def extract(first, count, r):
        @pl.loop(0, count, unroll=4)
        def _(i):
            row = H[first + i, pl.ds(r, nt, stride=2), :]
            X[r, pl.ds(pl.multiple_of((first + i) * nt, nt), nt), :] = row

    def row_copy(r, j, first, count, send, recv):
        start = pl.multiple_of((peer(j) * ng + first) * nt, nt)
        land = pl.multiple_of((1 + 2 * src + r) * pitch + first * nt, 8)
        return pltpu.make_async_remote_copy(
            src_ref=X.at[r, pl.ds(start, count * nt)],
            dst_ref=R.at[pl.ds(land, count * nt)],
            send_sem=send, recv_sem=recv,
            device_id={"src": peer(j)}, device_id_type=MESH,
        )

    def pass0(k, j):
        return row_copy(upper, j, k * s0, s0, y_send.at[j, k], y_recv.at[j, k])

    def pass1(k, j, first, count):
        return row_copy(1 - upper, j, first, count, z_send.at[j, k], z_recv.at[j, k])

    for k in range(k0):
        for j in far:
            load(j, k).wait()
            extract(peer(j) * ng + k * s0, s0, upper)
            if k == 0 and j == far[0]:
                pl.semaphore_wait(barrier, (n - 1) + (nv - 1))
            pass0(k, j).start()

    for j in far:
        extract(peer(j) * ng, ng, 1 - upper)

    def each_chunk(low, high, body):
        @pl.loop(low, min(high, k1 - 2))
        def _(k):
            body(k, k * GROUP, GROUP)

        for k in range(k1 - 2, high):
            body(k, ng - k1 + k, 1)

    def start_pass1(k, first, count):
        for j in far:
            pass1(k, j, first, count).start()

    each_chunk(0, k1, start_pass1)

    def weight_copy():
        return pltpu.make_async_remote_copy(
            src_ref=cot_ref.at[pl.ds(2, 2)], dst_ref=low, send_sem=w_send, recv_sem=w_recv,
            device_id={"vtx": (v + 1) % nv}, device_id_type=MESH,
        )

    @pl.when(v < nv - 1)
    def _():
        weight_copy().start()

    for k in range(k0):
        load(1, k).wait()
    for r in range(2):
        extract(peer(1) * ng, ng, r)

    def partner(r):
        return row_copy(r, 1, 0, ng, p_send.at[r], p_recv.at[r])

    for r in range(2):
        partner(r).start()

    for k in range(k0):
        load(0, k).wait()

    @pl.loop(0, ng)
    def _(s):
        for r in range(2):
            row = H[src * ng + s, pl.ds(r, nt, stride=2), :]
            R[pl.ds(pl.multiple_of((1 + 2 * src + r) * pitch + s * nt, 8), nt), :] = row

    @pl.when(v == 0)
    def _():
        R[pl.ds(0, ng * nt), :] = jnp.zeros((ng * nt, LANES), F32)

    @pl.when(v == nv - 1)
    def _():
        R[pl.ds(9 * pitch, ng * nt), :] = jnp.zeros((ng * nt, LANES), F32)

    def halo(up, k):
        first = k * s0 * nt
        out = (8 if up else 1) * pitch + first
        land = (0 if up else 9) * pitch + first
        to = (v + 1) % nv if up else (v + nv - 1) % nv
        return pltpu.make_async_remote_copy(
            src_ref=R.at[pl.ds(out, s0 * nt)], dst_ref=R.at[pl.ds(land, s0 * nt)],
            send_sem=h_send.at[up, k], recv_sem=h_recv.at[up, k],
            device_id={"vtx": to}, device_id_type=MESH,
        )

    def weights():
        cot_load.wait()
        idx_load.wait()

        @pl.when(v > 0)
        def _():
            weight_copy().wait_recv()

        shape = (ROWS, width)
        rows = lax.broadcasted_iota(jnp.int32, shape, 0)
        cols = lax.broadcasted_iota(jnp.int32, shape, 1)
        inside_col = cols < width - 1
        inside_row = rows + v * ROWS < total_rows - 1
        last = rows == ROWS - 1
        below = jnp.broadcast_to(v > 0, shape)
        W[0] = jnp.where(inside_col, cot[1], 0.0)
        W[1] = jnp.where(inside_row, cot[2], 0.0)
        W[4] = jnp.where(inside_col & inside_row, cot[3], 0.0)
        W[2] = pltpu.roll(jnp.where(last, jnp.where(below, low[0], 0.0), W[1]), 1, 0)
        W[3] = pltpu.roll(jnp.where(last, jnp.where(below & inside_col, low[1], 0.0), W[4]), 1, 0)
        W[5] = pltpu.roll(W[0], 1, 1)
        W[6] = cot[0] + W[0] + W[5] + W[1] + W[2] + W[4] + pltpu.roll(W[3], 1, 1)
        W[4] = pltpu.roll(W[4], 1, 1)

    for r in range(2):
        partner(r).wait_recv()
    weights()
    for k in range(k0):
        for j in far:
            pass0(k, j).wait_recv()

        @pl.when(v < nv - 1)
        def _():
            halo(1, k).start()

        @pl.when(v > 0)
        def _():
            halo(0, k).start()

    lane = lax.broadcasted_iota(jnp.int32, (ROWS, LANES), 1)
    flat = lax.broadcasted_iota(jnp.int32, (ROWS, LANES), 0) * width + lane
    first_lane, last_lane = lane == 0, lane == LANES - 1

    def chunk(k, first, count):
        tiles_per = BLOCK // count
        for j in far:
            pass1(k, j, first, count).wait_recv()
        spots = [idx_ref[src * ng + first + i] - v * (ROWS * width) for i in range(count)]

        def block(b, sums):
            sums = list(sums)
            t0 = b * tiles_per

            def weight(m, t):
                return W[m, :, pl.ds(pl.multiple_of(t * LANES, LANES), LANES)]

            before = (t0 + nt - 1) % nt
            after = (t0 + tiles_per) % nt
            tiles = [t0 + i for i in range(tiles_per)]
            for i in range(count):
                base = (first + i) * nt

                def field(shift, t):
                    return R[pl.ds((1 + shift) * pitch + base + t, ROWS, stride=pitch), :]

                mids = [field(0, t) for t in tiles]
                ups = [field(1, t) for t in tiles]
                downs = [field(-1, t) for t in tiles]
                p = [weight(5, t) * m + weight(4, t) * u for t, m, u in zip(tiles, mids, ups)]
                q = [weight(0, t) * m + weight(3, t) * d for t, m, d in zip(tiles, mids, downs)]
                p.append(weight(5, after) * field(0, after) + weight(4, after) * field(1, after))
                q.insert(0, weight(0, before) * field(0, before) + weight(3, before) * field(-1, before))
                for c, t in enumerate(tiles):
                    right = pltpu.roll(jnp.where(first_lane, p[c + 1], p[c]), LANES - 1, 1)
                    left = pltpu.roll(jnp.where(last_lane, q[c], q[c + 1]), 1, 1)
                    d = weight(6, t) * mids[c] - weight(1, t) * ups[c] - weight(2, t) * downs[c]
                    d = d - right - left
                    d = d - jnp.where(flat == spots[i] - t * LANES, F32(amplitude), F32(0.0))
                    sums[i] = sums[i] + d * d
                    D[first + i, :, pl.ds(pl.multiple_of(t * LANES, LANES), LANES)] = d
            return tuple(sums)

        zero = jnp.zeros((ROWS, LANES), F32)
        sums = lax.fori_loop(0, nt // tiles_per, block, (zero,) * count)
        for i in range(count):
            sq[pl.ds(first + i, 1), :] = jnp.sum(sums[i], axis=0, keepdims=True)

    cuts = [0, s0 // GROUP, k1]
    for k in range(k0):
        @pl.when(v > 0)
        def _():
            halo(1, k).wait_recv()

        @pl.when(v < nv - 1)
        def _():
            halo(0, k).wait_recv()

        each_chunk(cuts[k], cuts[k + 1], chunk)

    def share(to, slot):
        return pltpu.make_async_remote_copy(
            src_ref=sq, dst_ref=G.at[slot], send_sem=s_send.at[to], recv_sem=s_recv.at[slot],
            device_id={"vtx": to}, device_id_type=MESH,
        )

    @pl.loop(1, nv)
    def _(o):
        share((v + o) % nv, v).start()

    G[v] = sq[...]
    for j in far:
        for k in range(k0):
            pass0(k, j).wait_send()

    def end_pass1(k, first, count):
        for j in far:
            pass1(k, j, first, count).wait_send()

    each_chunk(0, k1, end_pass1)
    for r in range(2):
        partner(r).wait_send()

    @pl.when(v < nv - 1)
    def _():
        weight_copy().wait_send()
        for k in range(k0):
            halo(1, k).wait_send()

    @pl.when(v > 0)
    def _():
        for k in range(k0):
            halo(0, k).wait_send()

    @pl.loop(1, nv)
    def _(o):
        share((v + o) % nv, (v + o) % nv).wait_recv()

    total = lax.fori_loop(0, nv, lambda i, t: t + G[i], jnp.zeros((ng, LANES), F32))
    total = jnp.sum(total, axis=1, keepdims=True)
    norms = jnp.sqrt(total / (total_rows * width) + 1e-06)
    norm_ref[...] = jnp.broadcast_to(norms, (ng, LANES))

    @pl.loop(1, nv)
    def _(o):
        share((v + o) % nv, v).wait_send()


def scale(ng, nt, d_ref, n_ref, out_ref, norm_ref, O, sem):
    lane = lax.broadcasted_iota(jnp.int32, (ng, ng), 1)
    row = lax.broadcasted_iota(jnp.int32, (ng, ng), 0)

    def put(s):
        return pltpu.make_async_copy(O.at[s], out_ref.at[s], sem.at[s])

    @pl.loop(0, ng)
    def _(s):
        factor = jnp.broadcast_to(1.0 / n_ref[pl.ds(s, 1), :], (ROWS, LANES))
        for t in range(nt):
            at = pl.ds(t * LANES, LANES)
            O[s, :, at] = d_ref[s, :, at] * factor
        put(s).start()

    norm_ref[...] = jnp.sum(jnp.where(lane == row, n_ref[:, :ng], 0.0), axis=0, keepdims=True)

    @pl.loop(0, ng)
    def _(s):
        put(s).wait()


def on_device(n, nv, heat, cotan, source_index):
    sources, rpd, width = heat.shape
    assert rpd == 2 and cotan.shape[1] == ROWS and n % 2 == 0
    ng = sources // n
    nt = width // LANES
    pitch = -(-(ng * nt) // 64) * 64 + 8
    amplitude = math.sqrt(ROWS * nv * width) / 8.0
    tiled = heat.reshape(sources, rpd, nt, LANES).transpose(0, 2, 1, 3)
    tiled = tiled.reshape(sources, rpd * nt, LANES)
    dma = pltpu.SemaphoreType.DMA
    k0, k1 = 2, ng // GROUP + 1
    defect, norms = pl.pallas_call(
        functools.partial(kernel, n, nv, ng, width, pitch, amplitude),
        out_shape=(
            jax.ShapeDtypeStruct((ng, ROWS, width), F32),
            jax.ShapeDtypeStruct((ng, LANES), F32),
        ),
        in_specs=[
            pl.BlockSpec(memory_space=pltpu.HBM),
            pl.BlockSpec(memory_space=pltpu.HBM),
            pl.BlockSpec(memory_space=pltpu.HBM),
        ],
        out_specs=(
            pl.BlockSpec(memory_space=pltpu.VMEM),
            pl.BlockSpec(memory_space=pltpu.VMEM),
        ),
        scratch_shapes=[
            pltpu.SMEM((sources,), jnp.int32),
            pltpu.VMEM((sources, rpd * nt, LANES), F32),
            pltpu.VMEM((rpd, sources * nt, LANES), F32),
            pltpu.VMEM((10 * pitch, LANES), F32),
            pltpu.VMEM((7, ROWS, width), F32),
            pltpu.VMEM((4, ROWS, width), F32),
            pltpu.VMEM((2, ROWS, width), F32),
            pltpu.VMEM((ng, LANES), F32),
            pltpu.VMEM((nv, ng, LANES), F32),
            dma, dma((n, k0)), dma,
            dma((n, k0)), dma((n, k0)), dma((n, k1)), dma((n, k1)),
            dma((2,)), dma((2,)), dma((2, k0)), dma((2, k0)),
            dma, dma, dma((nv,)), dma((nv,)),
        ],
        compiler_params=pltpu.CompilerParams(
            collective_id=0, has_side_effects=True, vmem_limit_bytes=24 * 2**20
        ),
    )(*(pltpu.with_memory_space_constraint(x, pltpu.HBM) for x in (source_index, tiled, cotan)))
    out, norms = pl.pallas_call(
        functools.partial(scale, ng, nt),
        out_shape=(
            jax.ShapeDtypeStruct((ng, ROWS, width), F32),
            jax.ShapeDtypeStruct((1, ng), F32),
        ),
        in_specs=[pl.BlockSpec(memory_space=pltpu.VMEM)] * 2,
        out_specs=(
            pl.BlockSpec(memory_space=pltpu.HBM),
            pl.BlockSpec(memory_space=pltpu.VMEM),
        ),
        scratch_shapes=[pltpu.VMEM((ng, ROWS, width), F32), dma((ng,))],
        compiler_params=pltpu.CompilerParams(vmem_limit_bytes=16 * 2**20),
    )(defect, norms)
    return (out, norms.reshape(ng))


def solution(mesh):
    n, nv = mesh.shape["src"], mesh.shape["vtx"]
    return jax.shard_map(
        functools.partial(on_device, n, nv),
        mesh=mesh,
        in_specs=(P(None, ("vtx", "src"), None), P(None, "vtx", None), P()),
        out_specs=(P("src", "vtx", None), P("src")),
        check_vma=False,
    )
```

```python
import functools
import math

import jax
import jax.numpy as jnp
from jax import lax
from jax.experimental import pallas as pl
from jax.experimental.pallas import tpu as pltpu
from jax.sharding import PartitionSpec as P

MESH = pl.DeviceIdType.MESH
CUTS = 4
F32 = jnp.float32
LANES = 128
ROWS = 8
BLOCK = 32
GROUP = 2


def kernel(
    n, nv, ng, width, pitch, amplitude,
    idx_hbm, heat_ref, cot_ref, D, norm_ref,
    idx_ref, H, X, R, W, cot, low, sq, packed, G,
    idx_sem, load_sem, cot_sem, y_send, y_recv, z_send, z_recv, p_send, p_recv,
    h_send, h_recv, w_send, w_recv, s_send, s_recv,
):
    v = lax.axis_index("vtx")
    src = lax.axis_index("src")
    nt = width // LANES
    k0, k1 = CUTS, ng // GROUP + 1
    s0 = ng // k0
    total_rows = nv * ROWS
    far = list(range(2, n))
    upper = (src * 2) // n

    def peer(j):
        return ((src // 2 + j // 2) % (n // 2)) * 2 + (src + j) % 2

    def load(j, k):
        at = pl.ds(peer(j) * ng + k * s0, s0)
        return pltpu.make_async_copy(heat_ref.at[at], H.at[at], load_sem.at[j, k])

    for j in far:
        load(j, 0).start()
    barrier = pltpu.get_barrier_semaphore()
    for j in range(1, n):
        pl.semaphore_signal(barrier, inc=1, device_id={"src": peer(j)}, device_id_type=MESH)

    @pl.loop(1, nv)
    def _(o):
        pl.semaphore_signal(barrier, inc=1, device_id={"vtx": (v + o) % nv}, device_id_type=MESH)

    def extract(first, count, r):
        @pl.loop(0, count, unroll=4)
        def _(i):
            row = H[first + i, pl.ds(r, nt, stride=2), :]
            X[r, pl.ds(pl.multiple_of((first + i) * nt, nt), nt), :] = row

    def row_copy(r, j, first, count, send, recv):
        start = pl.multiple_of((peer(j) * ng + first) * nt, nt)
        land = pl.multiple_of((1 + 2 * src + r) * pitch + first * nt, 8)
        return pltpu.make_async_remote_copy(
            src_ref=X.at[r, pl.ds(start, count * nt)],
            dst_ref=R.at[pl.ds(land, count * nt)],
            send_sem=send, recv_sem=recv,
            device_id={"src": peer(j)}, device_id_type=MESH,
        )

    def pass0(k, j):
        return row_copy(upper, j, k * s0, s0, y_send.at[j, k], y_recv.at[j, k])

    def pass1(k, j, first, count):
        return row_copy(1 - upper, j, first, count, z_send.at[j, k], z_recv.at[j, k])

    load(far[0], 0).wait()
    for k in range(1, k0):
        for j in far:
            load(j, k).start()
    for j in (1, 0):
        for k in range(k0):
            load(j, k).start()
    cot_load = pltpu.make_async_copy(cot_ref, cot, cot_sem)
    cot_load.start()
    idx_load = pltpu.make_async_copy(idx_hbm, idx_ref, idx_sem)
    idx_load.start()

    for k in range(k0):
        for j in far:
            if k > 0 or j != far[0]:
                load(j, k).wait()
            extract(peer(j) * ng + k * s0, s0, upper)
            if k == 0 and j == far[0]:
                pl.semaphore_wait(barrier, (n - 1) + (nv - 1))
            pass0(k, j).start()

    for j in far:
        extract(peer(j) * ng, ng, 1 - upper)

    def each_chunk(low, high, body):
        @pl.loop(low, min(high, k1 - 2))
        def _(k):
            body(k, k * GROUP, GROUP)

        for k in range(k1 - 2, high):
            body(k, ng - k1 + k, 1)

    def start_pass1(k, first, count):
        for j in far:
            pass1(k, j, first, count).start()

    each_chunk(0, k1, start_pass1)

    def weight_copy():
        return pltpu.make_async_remote_copy(
            src_ref=cot_ref.at[pl.ds(2, 2)], dst_ref=low, send_sem=w_send, recv_sem=w_recv,
            device_id={"vtx": (v + 1) % nv}, device_id_type=MESH,
        )

    @pl.when(v < nv - 1)
    def _():
        weight_copy().start()

    for k in range(k0):
        load(1, k).wait()
    for r in range(2):
        extract(peer(1) * ng, ng, r)

    def partner(r):
        return row_copy(r, 1, 0, ng, p_send.at[r], p_recv.at[r])

    for r in range(2):
        partner(r).start()

    for k in range(k0):
        load(0, k).wait()

    @pl.loop(0, ng)
    def _(s):
        for r in range(2):
            row = H[src * ng + s, pl.ds(r, nt, stride=2), :]
            R[pl.ds(pl.multiple_of((1 + 2 * src + r) * pitch + s * nt, 8), nt), :] = row

    @pl.when(v == 0)
    def _():
        R[pl.ds(0, ng * nt), :] = jnp.zeros((ng * nt, LANES), F32)

    @pl.when(v == nv - 1)
    def _():
        R[pl.ds(9 * pitch, ng * nt), :] = jnp.zeros((ng * nt, LANES), F32)

    def halo(up, k):
        first = k * s0 * nt
        out = (8 if up else 1) * pitch + first
        land = (0 if up else 9) * pitch + first
        to = (v + 1) % nv if up else (v + nv - 1) % nv
        return pltpu.make_async_remote_copy(
            src_ref=R.at[pl.ds(out, s0 * nt)], dst_ref=R.at[pl.ds(land, s0 * nt)],
            send_sem=h_send.at[up, k], recv_sem=h_recv.at[up, k],
            device_id={"vtx": to}, device_id_type=MESH,
        )

    def weights():
        cot_load.wait()
        idx_load.wait()

        @pl.when(v > 0)
        def _():
            weight_copy().wait_recv()

        shape = (ROWS, width)
        rows = lax.broadcasted_iota(jnp.int32, shape, 0)
        cols = lax.broadcasted_iota(jnp.int32, shape, 1)
        inside_col = cols < width - 1
        inside_row = rows + v * ROWS < total_rows - 1
        last = rows == ROWS - 1
        below = jnp.broadcast_to(v > 0, shape)
        W[0] = jnp.where(inside_col, cot[1], 0.0)
        W[1] = jnp.where(inside_row, cot[2], 0.0)
        W[4] = jnp.where(inside_col & inside_row, cot[3], 0.0)
        W[2] = pltpu.roll(jnp.where(last, jnp.where(below, low[0], 0.0), W[1]), 1, 0)
        W[3] = pltpu.roll(jnp.where(last, jnp.where(below & inside_col, low[1], 0.0), W[4]), 1, 0)
        W[5] = pltpu.roll(W[0], 1, 1)
        W[6] = cot[0] + W[0] + W[5] + W[1] + W[2] + W[4] + pltpu.roll(W[3], 1, 1)
        W[4] = pltpu.roll(W[4], 1, 1)

    for r in range(2):
        partner(r).wait_recv()
    weights()
    for k in range(k0):
        for j in far:
            pass0(k, j).wait_recv()

        @pl.when(v < nv - 1)
        def _():
            halo(1, k).start()

        @pl.when(v > 0)
        def _():
            halo(0, k).start()

    lane = lax.broadcasted_iota(jnp.int32, (ROWS, LANES), 1)
    flat = lax.broadcasted_iota(jnp.int32, (ROWS, LANES), 0) * width + lane
    first_lane, last_lane = lane == 0, lane == LANES - 1

    def chunk(k, first, count):
        tiles_per = BLOCK // count
        for j in far:
            pass1(k, j, first, count).wait_recv()
        spots = [idx_ref[src * ng + first + i] - v * (ROWS * width) for i in range(count)]

        def block(b, sums):
            sums = list(sums)
            t0 = b * tiles_per

            def weight(m, t):
                return W[m, :, pl.ds(pl.multiple_of(t * LANES, LANES), LANES)]

            before = (t0 + nt - 1) % nt
            after = (t0 + tiles_per) % nt
            tiles = [t0 + i for i in range(tiles_per)]
            for i in range(count):
                base = (first + i) * nt

                def field(shift, t):
                    return R[pl.ds((1 + shift) * pitch + base + t, ROWS, stride=pitch), :]

                mids = [field(0, t) for t in tiles]
                ups = [field(1, t) for t in tiles]
                downs = [field(-1, t) for t in tiles]
                p = [weight(5, t) * m + weight(4, t) * u for t, m, u in zip(tiles, mids, ups)]
                q = [weight(0, t) * m + weight(3, t) * d for t, m, d in zip(tiles, mids, downs)]
                p.append(weight(5, after) * field(0, after) + weight(4, after) * field(1, after))
                q.insert(0, weight(0, before) * field(0, before) + weight(3, before) * field(-1, before))
                for c, t in enumerate(tiles):
                    right = pltpu.roll(jnp.where(first_lane, p[c + 1], p[c]), LANES - 1, 1)
                    left = pltpu.roll(jnp.where(last_lane, q[c], q[c + 1]), 1, 1)
                    d = weight(6, t) * mids[c] - weight(1, t) * ups[c] - weight(2, t) * downs[c]
                    d = d - right - left
                    d = d - jnp.where(flat == spots[i] - t * LANES, F32(amplitude), F32(0.0))
                    sums[i] = sums[i] + d * d
                    D[first + i, :, pl.ds(pl.multiple_of(t * LANES, LANES), LANES)] = d
            return tuple(sums)

        zero = jnp.zeros((ROWS, LANES), F32)
        sums = lax.fori_loop(0, nt // tiles_per, block, (zero,) * count)
        for i in range(count):
            sq[pl.ds(first + i, 1), :] = jnp.sum(sums[i], axis=0, keepdims=True)

    cuts = [k * s0 // GROUP for k in range(k0)] + [k1]
    for k in range(k0):
        @pl.when(v > 0)
        def _():
            halo(1, k).wait_recv()

        @pl.when(v < nv - 1)
        def _():
            halo(0, k).wait_recv()

        each_chunk(cuts[k], cuts[k + 1], chunk)

    def share(to, slot):
        return pltpu.make_async_remote_copy(
            src_ref=packed, dst_ref=G.at[slot], send_sem=s_send.at[to], recv_sem=s_recv.at[slot],
            device_id={"vtx": to}, device_id_type=MESH,
        )

    spot = lax.broadcasted_iota(jnp.int32, (ng, LANES), 1)
    on_spot = spot == lax.broadcasted_iota(jnp.int32, (ng, LANES), 0)
    totals = jnp.sum(sq[...], axis=1, keepdims=True)
    mine = jnp.sum(jnp.where(on_spot, totals, 0.0), axis=0, keepdims=True)
    packed[...] = mine

    @pl.loop(1, nv)
    def _(o):
        share((v + o) % nv, v).start()

    G[v] = mine
    for j in far:
        for k in range(k0):
            pass0(k, j).wait_send()

    def end_pass1(k, first, count):
        for j in far:
            pass1(k, j, first, count).wait_send()

    each_chunk(0, k1, end_pass1)
    for r in range(2):
        partner(r).wait_send()

    @pl.when(v < nv - 1)
    def _():
        weight_copy().wait_send()
        for k in range(k0):
            halo(1, k).wait_send()

    @pl.when(v > 0)
    def _():
        for k in range(k0):
            halo(0, k).wait_send()

    @pl.loop(1, nv)
    def _(o):
        share((v + o) % nv, (v + o) % nv).wait_recv()

    total = lax.fori_loop(0, nv, lambda i, t: t + G[i], jnp.zeros((1, LANES), F32))
    norm_ref[...] = jnp.sqrt(total / (total_rows * width) + 1e-06)

    @pl.loop(1, nv)
    def _(o):
        share((v + o) % nv, v).wait_send()


def scale(ng, nt, d_ref, n_ref, out_ref, norm_ref, F, O, sem):
    lane = lax.broadcasted_iota(jnp.int32, (ng, LANES), 1)
    row = lax.broadcasted_iota(jnp.int32, (ng, LANES), 0)
    inverse = jnp.sum(jnp.where(lane == row, 1.0 / n_ref[...], 0.0), axis=1, keepdims=True)
    F[...] = jnp.broadcast_to(inverse, (ng, LANES))
    norm_ref[...] = n_ref[:, :ng]

    def put(s):
        return pltpu.make_async_copy(O.at[s], out_ref.at[s], sem.at[s])

    @pl.loop(0, ng)
    def _(s):
        factor = jnp.broadcast_to(F[pl.ds(s, 1), :], (ROWS, LANES))
        for t in range(nt):
            at = pl.ds(t * LANES, LANES)
            O[s, :, at] = d_ref[s, :, at] * factor
        put(s).start()

    @pl.loop(0, ng)
    def _(s):
        put(s).wait()


def on_device(n, nv, heat, cotan, source_index):
    sources, rpd, width = heat.shape
    assert rpd == 2 and cotan.shape[1] == ROWS and n % 2 == 0
    ng = sources // n
    assert ng <= LANES and ng % (CUTS * GROUP) == 0
    nt = width // LANES
    pitch = -(-(ng * nt) // 64) * 64 + 8
    amplitude = math.sqrt(ROWS * nv * width) / 8.0
    tiled = heat.reshape(sources, rpd, nt, LANES).transpose(0, 2, 1, 3)
    tiled = tiled.reshape(sources, rpd * nt, LANES)
    dma = pltpu.SemaphoreType.DMA
    k0, k1 = CUTS, ng // GROUP + 1
    defect, norms = pl.pallas_call(
        functools.partial(kernel, n, nv, ng, width, pitch, amplitude),
        out_shape=(
            jax.ShapeDtypeStruct((ng, ROWS, width), F32),
            jax.ShapeDtypeStruct((1, LANES), F32),
        ),
        in_specs=[
            pl.BlockSpec(memory_space=pltpu.HBM),
            pl.BlockSpec(memory_space=pltpu.HBM),
            pl.BlockSpec(memory_space=pltpu.HBM),
        ],
        out_specs=(
            pl.BlockSpec(memory_space=pltpu.VMEM),
            pl.BlockSpec(memory_space=pltpu.VMEM),
        ),
        scratch_shapes=[
            pltpu.SMEM((sources,), jnp.int32),
            pltpu.VMEM((sources, rpd * nt, LANES), F32),
            pltpu.VMEM((rpd, sources * nt, LANES), F32),
            pltpu.VMEM((10 * pitch, LANES), F32),
            pltpu.VMEM((7, ROWS, width), F32),
            pltpu.VMEM((4, ROWS, width), F32),
            pltpu.VMEM((2, ROWS, width), F32),
            pltpu.VMEM((ng, LANES), F32),
            pltpu.VMEM((1, LANES), F32),
            pltpu.VMEM((nv, 1, LANES), F32),
            dma, dma((n, k0)), dma,
            dma((n, k0)), dma((n, k0)), dma((n, k1)), dma((n, k1)),
            dma((2,)), dma((2,)), dma((2, k0)), dma((2, k0)),
            dma, dma, dma((nv,)), dma((nv,)),
        ],
        compiler_params=pltpu.CompilerParams(
            collective_id=0, has_side_effects=True, vmem_limit_bytes=24 * 2**20
        ),
    )(*(pltpu.with_memory_space_constraint(x, pltpu.HBM) for x in (source_index, tiled, cotan)))
    out, norms = pl.pallas_call(
        functools.partial(scale, ng, nt),
        out_shape=(
            jax.ShapeDtypeStruct((ng, ROWS, width), F32),
            jax.ShapeDtypeStruct((1, ng), F32),
        ),
        in_specs=[pl.BlockSpec(memory_space=pltpu.VMEM)] * 2,
        out_specs=(
            pl.BlockSpec(memory_space=pltpu.HBM),
            pl.BlockSpec(memory_space=pltpu.VMEM),
        ),
        scratch_shapes=[
            pltpu.VMEM((ng, LANES), F32), pltpu.VMEM((ng, ROWS, width), F32), dma((ng,))
        ],
        compiler_params=pltpu.CompilerParams(vmem_limit_bytes=16 * 2**20),
    )(defect, norms)
    return (out, norms.reshape(ng))


def solution(mesh):
    n, nv = mesh.shape["src"], mesh.shape["vtx"]
    return jax.shard_map(
        functools.partial(on_device, n, nv),
        mesh=mesh,
        in_specs=(P(None, ("vtx", "src"), None), P(None, "vtx", None), P()),
        out_specs=(P("src", "vtx", None), P("src")),
        check_vma=False,
    )
```
